16 devices in a mesh: ens: 4 (over z, y), sp: 4 (over x, core).
Axes of the slice: x: 2, y: 2, z: 2, core: 2. Of those that a mesh axis runs over, the one named last changes fastest.
Arguments:
- x_seq: bfloat16 [32768, 128], P(('ens', 'sp')), parts along dimension 0
- w_past: bfloat16 [2, 10, 128, 256], replicated
- w_now: bfloat16 [2, 10, 128, 256], replicated
- b_conv: float32 [2, 10, 256], replicated
- w_res: bfloat16 [2, 10, 128, 128], replicated
- w_skip: bfloat16 [2, 10, 128, 128], replicated
- w_out1: bfloat16 [128, 128], replicated
- b_out1: float32 [128], replicated
- w_out2: bfloat16 [128, 256], replicated
- b_out2: float32 [256], replicated
Outputs:
- output 1: float32 [32768, 256], P(('ens', 'sp')), parts along dimension 0
- output 2: bfloat16 [32768, 128], P(('ens', 'sp')), parts along dimension 0
There are 4 independent parts. The reference program is written for one: setup_inputs(seed, part) draws one part's arguments, and reference() takes and returns one part's arrays. A program takes and returns all parts, laid end to end along the dimension named above; an argument that names none is the same for every part.
All inputs are finite; a program needn't handle non-finite values.
Results may differ from the reference program's by a relative error of at most 0.0142219.
Values are sent between devices in bfloat16 or wider.
A program may use at most 1 GiB of HBM per device.

```python
import jax
import jax.numpy as jnp
from jax import lax

SEQ_LEN = 8192
RES_CH = 128
GATE_CH = 128
SKIP_CH = 128
CLASSES = 256
DIL_CYCLE = 10
STACKS = 2
LAYERS_ALL = STACKS * DIL_CYCLE


def setup_inputs(seed: int = 0, part: int = 0) -> dict:
    root_key = jax.random.key(seed)
    subkeys = jax.random.split(root_key, 10)
    seq_key = jax.random.fold_in(subkeys[0], part)
    conv_shape = (STACKS, DIL_CYCLE, RES_CH, 2 * GATE_CH)
    conv_scale = (2 * RES_CH) ** -0.5
    proj_scale = 2.0 * (GATE_CH * LAYERS_ALL) ** -0.5
    head_scale = 2.0 * SKIP_CH ** -0.5
    x_seq = jax.random.normal(seq_key, (SEQ_LEN, RES_CH), jnp.float32)
    w_past = jax.random.normal(subkeys[1], conv_shape, jnp.float32) * conv_scale
    w_now = jax.random.normal(subkeys[2], conv_shape, jnp.float32) * conv_scale
    b_conv = jax.random.normal(subkeys[3], (STACKS, DIL_CYCLE, 2 * GATE_CH), jnp.float32) * 0.5
    w_res = jax.random.normal(subkeys[4], (STACKS, DIL_CYCLE, GATE_CH, RES_CH), jnp.float32) * proj_scale
    w_skip = jax.random.normal(subkeys[5], (STACKS, DIL_CYCLE, GATE_CH, SKIP_CH), jnp.float32) * proj_scale
    w_out1 = jax.random.normal(subkeys[6], (SKIP_CH, SKIP_CH), jnp.float32) * head_scale
    b_out1 = jax.random.normal(subkeys[7], (SKIP_CH,), jnp.float32) * 0.5
    w_out2 = jax.random.normal(subkeys[8], (SKIP_CH, CLASSES), jnp.float32) * head_scale
    b_out2 = jax.random.normal(subkeys[9], (CLASSES,), jnp.float32) * 0.5
    return {
        "x_seq": x_seq.astype(jnp.bfloat16),
        "w_past": w_past.astype(jnp.bfloat16),
        "w_now": w_now.astype(jnp.bfloat16),
        "b_conv": b_conv,
        "w_res": w_res.astype(jnp.bfloat16),
        "w_skip": w_skip.astype(jnp.bfloat16),
        "w_out1": w_out1.astype(jnp.bfloat16),
        "b_out1": b_out1,
        "w_out2": w_out2.astype(jnp.bfloat16),
        "b_out2": b_out2,
    }


def reference(x_seq, w_past, w_now, b_conv, w_res, w_skip, w_out1, b_out1, w_out2, b_out2):
    def stack_body(carry, stack_w):
        hidden, skip_sum = carry
        past_w, now_w, conv_b, res_w, skip_w = stack_w
        for layer_pos in range(DIL_CYCLE):
            dilation = 2 ** layer_pos
            shifted = jnp.concatenate([jnp.zeros((dilation, RES_CH), hidden.dtype), hidden[:SEQ_LEN - dilation]], axis=0)
            pre_act = (jnp.dot(shifted, past_w[layer_pos], preferred_element_type=jnp.float32)
                       + jnp.dot(hidden, now_w[layer_pos], preferred_element_type=jnp.float32)
                       + conv_b[layer_pos])
            gated = (jnp.tanh(pre_act[:, :GATE_CH]) * jax.nn.sigmoid(pre_act[:, GATE_CH:])).astype(jnp.bfloat16)
            hidden = (hidden.astype(jnp.float32) + jnp.dot(gated, res_w[layer_pos], preferred_element_type=jnp.float32)).astype(jnp.bfloat16)
            skip_sum = skip_sum + jnp.dot(gated, skip_w[layer_pos], preferred_element_type=jnp.float32)
        return (hidden, skip_sum), None

    skip_init = jnp.zeros((SEQ_LEN, SKIP_CH), jnp.float32)
    (hidden, skip_sum), _ = lax.scan(stack_body, (x_seq, skip_init), (w_past, w_now, b_conv, w_res, w_skip))
    skip_act = jax.nn.relu(skip_sum).astype(jnp.bfloat16)
    mid_act = jax.nn.relu(jnp.dot(skip_act, w_out1, preferred_element_type=jnp.float32) + b_out1).astype(jnp.bfloat16)
    logits = jnp.dot(mid_act, w_out2, preferred_element_type=jnp.float32) + b_out2
    return (logits, hidden)
```

```python
import functools

import jax
import jax.numpy as jnp
from jax import lax
from jax.experimental import pallas as pl
from jax.experimental.pallas import tpu as pltpu
from jax.sharding import PartitionSpec as P

F32 = jnp.float32
BF16 = jnp.bfloat16
T = 2048
C = 128
EXT = 128
PAD = 64
BASE = PAD + EXT
TILE = 256
HBM = pl.BlockSpec(memory_space=pltpu.HBM)
SENDS = (("x", 128), ("h7", 128), ("h8", 256), ("h9", 512), ("h10", 128), ("h17", 128), ("h18", 256), ("h19", 512))
SLOT = {name: i for i, (name, _) in enumerate(SENDS)}
ROWS = dict(SENDS)
OFFSET = {}
_at = 0
for _name, _rows in SENDS:
    OFFSET[_name] = _at
    _at += _rows
HALO_ROWS = _at


def stack_kernel(x_ref, wp_ref, wn_ref, b_ref, wr_ref, ws_ref, a_out, h_out,
                 hid, pre, skip, keep, send_buf, recv_buf, wp, wn, wr, ws, bias,
                 load_sem, w_sem, send_sem, recv_sem):
    sp = lax.axis_index("sp")
    right = lax.rem(sp + 1, 4)
    left = lax.rem(sp + 3, 4)
    first = sp == 0

    barrier = pltpu.get_barrier_semaphore()
    pl.semaphore_signal(barrier, inc=1, device_id={"sp": left}, device_id_type=pl.DeviceIdType.MESH)

    def remote(name, src):
        rows = ROWS[name]
        return pltpu.make_async_remote_copy(
            src_ref=src,
            dst_ref=recv_buf.at[pl.ds(OFFSET[name], rows)],
            send_sem=send_sem.at[SLOT[name]],
            recv_sem=recv_sem.at[SLOT[name]],
            device_id={"sp": right},
            device_id_type=pl.DeviceIdType.MESH,
        )

    def send_of(name):
        if name == "x":
            return remote(name, x_ref.at[pl.ds(T - EXT, EXT)])
        return remote(name, send_buf.at[pl.ds(OFFSET[name], ROWS[name])])

    load_x = pltpu.make_async_copy(x_ref, hid.at[pl.ds(BASE, T)], load_sem.at[0])
    load_b = pltpu.make_async_copy(b_ref, bias, load_sem.at[1])
    load_pre = pltpu.make_async_copy(x_ref.at[pl.ds(0, 128)], pre.at[pl.ds(BASE, 128)], load_sem.at[2])
    groups = ((0, 0, 1), (0, 1, 9), (1, 0, 10))
    w_loads = []
    for g, (s, k0, n) in enumerate(groups):
        w_loads.append([
            pltpu.make_async_copy(src.at[s, pl.ds(k0, n)], dst.at[s, pl.ds(k0, n)], w_sem.at[g, i])
            for i, (src, dst) in enumerate(((wp_ref, wp), (wn_ref, wn), (wr_ref, wr), (ws_ref, ws)))
        ])
    load_x.start()
    load_b.start()
    for copies in w_loads:
        for copy in copies:
            copy.start()
    load_pre.start()
    hid[pl.ds(0, BASE), :] = jnp.zeros((BASE, C), BF16)
    pre[pl.ds(0, PAD), :] = jnp.zeros((PAD, C), BF16)

    pl.semaphore_wait(barrier, 1)
    send_of("x").start()

    def halo(name, lo, n):
        rows = recv_buf[pl.ds(OFFSET[name] + lo, n), :]
        return jnp.where(first, jnp.zeros_like(rows), rows)

    def tile(l, r0, r1, buf, past_of, skip_from, skip_init=False, zero_to=None, tail=None):
        s, k = divmod(l, 10)
        n = r1 - r0
        now = buf[pl.ds(BASE + r0, n), :]
        past = past_of(r0, n)
        w = jnp.concatenate([wp[s, k], wn[s, k]], axis=0)
        z = jnp.dot(jnp.concatenate([past, now], axis=1), w, preferred_element_type=F32)
        z = z + bias[s, pl.ds(k, 1), :]
        gate = 0.5 * jnp.tanh(0.5 * z[:, C:]) + 0.5
        g = (jnp.tanh(z[:, :C]) * gate).astype(BF16)
        out = jnp.dot(g, jnp.concatenate([wr[s, k], ws[s, k]], axis=1), preferred_element_type=F32)
        new = (now.astype(F32) + out[:, :C]).astype(BF16)
        if zero_to is not None and r0 < zero_to:
            m = zero_to - r0
            head = jnp.where(first, jnp.zeros((m, C), BF16), new[:m])
            new = head if m == n else jnp.concatenate([head, new[m:]], axis=0)
        if l == 19:
            h_out[pl.ds(r0, n), :] = new
        else:
            buf[pl.ds(BASE + r0, n), :] = new
        if tail is not None and r1 > T - ROWS[tail]:
            cut = max(T - ROWS[tail] - r0, 0)
            send_buf[pl.ds(OFFSET[tail] + r0 + cut - (T - ROWS[tail]), n - cut), :] = new[cut:]
        lo = max(r0, skip_from)
        if lo < r1:
            add = out[lo - r0:, C:]
            rows = pl.ds(lo, r1 - lo)
            total = add if skip_init else skip[rows, :] + add
            if l == 19:
                a_out[rows, :] = jnp.maximum(total, 0.0).astype(BF16)
            else:
                skip[rows, :] = total

    def tiles(lo, hi, step=TILE):
        cuts = []
        r1 = hi
        while r1 > lo:
            r0 = max(lo, -(-r1 // step) * step - step)
            cuts.append((r0, r1))
            r1 = r0
        return cuts

    def past_in(buf, d):
        return lambda r0, n: buf[pl.ds(BASE + r0 - d, n), :]

    def past_halo(name, d):
        def get(r0, n):
            if r0 >= d:
                return hid[pl.ds(BASE + r0 - d, n), :]
            m = min(n, d - r0)
            part = halo(name, r0, m)
            if m == n:
                return part
            return jnp.concatenate([part, hid[pl.ds(BASE, n - m), :]], axis=0)
        return get

    def layer(l, lo, hi, skip_from, tail=None, halo_name=None, zero_to=None, buf=None):
        d = 2 ** (l % 10)
        buf = hid if buf is None else buf
        past = past_halo(halo_name, d) if halo_name else past_in(buf, d)
        cuts = tiles(lo, hi)
        for i, (r0, r1) in enumerate(cuts):
            due = list(pending)
            tile(l, r0, r1, buf, past, skip_from, skip_init=(l == 0), zero_to=zero_to, tail=tail)
            for name in due:
                send_of(name).start()
                pending.remove(name)
            if tail is not None and r0 <= T - ROWS[tail] < r1:
                pending.append(tail)

    pending = []

    def flush():
        for name in pending:
            send_of(name).start()
        pending.clear()

    load_x.wait()
    load_b.wait()
    for copy in w_loads[0]:
        copy.wait()
    layer(0, 0, T, 128)
    for copy in w_loads[1]:
        copy.wait()
    for l in range(1, 7):
        layer(l, 0, T, 128, tail="h7" if l == 6 else None)
    layer(7, 256, T, 128, tail="h8")
    layer(8, 512, T, 128, tail="h9")
    layer(9, 1024, T, 128, tail="h10")
    for copy in w_loads[2]:
        copy.wait()
    keep[...] = hid[pl.ds(BASE + 1024, 128), :]

    send_of("x").wait_recv()
    load_pre.wait()
    pre[pl.ds(PAD, EXT), :] = halo("x", 0, EXT)
    for k in range(7):
        layer(10 + k, 1024, T, 1152, tail="h17" if k == 6 else None)
        layer(k, -EXT, 128, 0, zero_to=0, buf=pre)
    layer(17, 1280, T, 0, tail="h18")
    layer(18, 1536, T, 0, tail="h19")

    hid[pl.ds(BASE, 128), :] = pre[pl.ds(BASE, 128), :]
    hid[pl.ds(BASE + 1024, 128), :] = keep[...]
    for l, hi in ((7, 256), (8, 512), (9, 1024)):
        send_of(f"h{l}").wait_recv()
        layer(l, 0, hi, 0, halo_name=f"h{l}")

    send_of("h10").wait_recv()
    hid[pl.ds(PAD, EXT), :] = halo("h10", 0, EXT)
    for l in range(10, 17):
        layer(l, -EXT, 1152, 0, zero_to=0)
    for l, hi in ((17, 1280), (18, 1536), (19, T)):
        send_of(f"h{l}").wait_recv()
        layer(l, 0, hi, 0, halo_name=f"h{l}")
    flush()
    for name, _ in SENDS:
        send_of(name).wait_send()


def head_kernel(a_ref, h_ref, w1_ref, c1_ref, w2_ref, c2_ref, y_ref, h_out):
    m = jnp.dot(a_ref[...], w1_ref[...], preferred_element_type=F32) + c1_ref[...]
    m = jnp.maximum(m, 0.0).astype(BF16)
    y_ref[...] = jnp.dot(m, w2_ref[...], preferred_element_type=F32) + c2_ref[...]
    h_out[...] = h_ref[...]


def solution(mesh):
    row_spec = P(("ens", "sp"), None)

    def local_stack(x_seq, w_past, w_now, b_conv, w_res, w_skip, w_out1, b_out1, w_out2, b_out2):
        vmem = pl.BlockSpec(memory_space=pltpu.VMEM)
        a, h = pl.pallas_call(
            stack_kernel,
            out_shape=(jax.ShapeDtypeStruct((T, C), BF16), jax.ShapeDtypeStruct((T, C), BF16)),
            in_specs=[HBM] * 6,
            out_specs=(vmem, vmem),
            scratch_shapes=[
                pltpu.VMEM((BASE + T, C), BF16),
                pltpu.VMEM((BASE + 128, C), BF16),
                pltpu.VMEM((T, C), F32),
                pltpu.VMEM((128, C), BF16),
                pltpu.VMEM((HALO_ROWS, C), BF16),
                pltpu.VMEM((HALO_ROWS, C), BF16),
                pltpu.VMEM((2, 10, C, 2 * C), BF16),
                pltpu.VMEM((2, 10, C, 2 * C), BF16),
                pltpu.VMEM((2, 10, C, C), BF16),
                pltpu.VMEM((2, 10, C, C), BF16),
                pltpu.VMEM((2, 10, 2 * C), F32),
                pltpu.SemaphoreType.DMA((3,)),
                pltpu.SemaphoreType.DMA((3, 4)),
                pltpu.SemaphoreType.DMA((len(SENDS),)),
                pltpu.SemaphoreType.DMA((len(SENDS),)),
            ],
            compiler_params=pltpu.CompilerParams(
                collective_id=0, has_side_effects=True, vmem_limit_bytes=65_600_000),
            name="stack",
        )(x_seq, w_past, w_now, b_conv, w_res, w_skip)
        step = 512
        rows = lambda width: pl.BlockSpec((step, width), lambda i: (i, 0))
        whole = lambda *shape: pl.BlockSpec(shape, lambda i: (0,) * len(shape))
        return pl.pallas_call(
            head_kernel,
            grid=(T // step,),
            out_shape=(jax.ShapeDtypeStruct((T, 2 * C), F32), jax.ShapeDtypeStruct((T, C), BF16)),
            in_specs=[rows(C), rows(C), whole(C, C), whole(1, C), whole(C, 2 * C), whole(1, 2 * C)],
            out_specs=(rows(2 * C), rows(C)),
            compiler_params=pltpu.CompilerParams(vmem_limit_bytes=16 * 1024 * 1024),
            name="head",
        )(a, h, w_out1, b_out1.reshape(1, C), w_out2, b_out2.reshape(1, 2 * C))

    return jax.shard_map(
        local_stack,
        mesh=mesh,
        in_specs=(row_spec, P(), P(), P(), P(), P(), P(), P(), P(), P()),
        out_specs=(row_spec, row_spec),
        check_vma=False,
    )
```
